8 devices in a mesh: col: 4 (over z, y, x), row: 2 (over core).
Axes of the slice: x: 2, y: 2, z: 1, core: 2. Of those that a mesh axis runs over, the one named last changes fastest.
Arguments:
- adjacency: bfloat16 [16384, 16384], P('row', 'col')
- x_init: float32 [16384, 128], P(('col', 'row'))
- teleport: float32 [16384, 128], P(('col', 'row'))
- dangling: int32 [16384], P(('col', 'row'))
- damping: float32 [32], replicated
Outputs:
- output 1: float32 [16384, 128], P(('col', 'row'))
- output 2: float32 [32, 128], replicated
All inputs are finite; a program needn't handle non-finite values.
Results may differ from the reference program's by a relative error of at most 0.001.
Values are sent between devices in bfloat16 or wider.
A program may use at most 1 GiB of HBM per device.

```python
import jax
import jax.numpy as jnp
from jax import lax

N = 16384
M = 128
K = 32
ROW_BLOCK = min(N, 512)
N_BLOCKS = N // ROW_BLOCK


def build_graph(key_edge, long_deg, band_width, dangling):
    col_ids = jnp.arange(N)
    is_live = dangling == 0

    def block_mask(block_id):
        row_ids = block_id * ROW_BLOCK + jnp.arange(ROW_BLOCK)
        rand_draw = jax.random.randint(jax.random.fold_in(key_edge, block_id), (ROW_BLOCK, N), 0, N)
        offset = (row_ids[:, None] - col_ids[None, :]) % N
        edge_mask = (rand_draw < long_deg[None, :]) | ((offset >= 1) & (offset <= band_width[None, :]))
        return edge_mask & is_live[None, :]

    def block_count(block_id):
        return jnp.sum(block_mask(block_id), axis=0, dtype=jnp.int32)

    out_deg = jnp.sum(lax.map(block_count, jnp.arange(N_BLOCKS)), axis=0)
    weight = 1.0 / jnp.maximum(out_deg, 1).astype(jnp.float32)

    def block_values(block_id):
        return jnp.where(block_mask(block_id), weight[None, :], 0.0).astype(jnp.bfloat16)

    return lax.map(block_values, jnp.arange(N_BLOCKS)).reshape(N, N)


def setup_inputs(seed: int = 0) -> dict:
    root = jax.random.key(seed)
    k_dang, k_deg, k_band, k_edge, k_start, k_tele, k_damp = jax.random.split(root, 7)
    dangling = (jax.random.randint(k_dang, (N,), 0, 5) == 0).astype(jnp.int32)
    long_deg = jnp.left_shift(1, jax.random.randint(k_deg, (N,), 1, 6))
    band_width = jax.random.randint(k_band, (N,), 1, 9)
    adjacency = build_graph(k_edge, long_deg, band_width, dangling)
    x_raw = jnp.exp(0.5 * jax.random.normal(k_start, (N, M), jnp.float32))
    x_init = x_raw / jnp.mean(x_raw, axis=0, keepdims=True)
    tele_raw = jnp.exp(1.5 * jax.random.normal(k_tele, (N, M), jnp.float32))
    teleport = tele_raw / jnp.mean(tele_raw, axis=0, keepdims=True)
    damping = jax.random.uniform(k_damp, (K,), jnp.float32, 0.8, 0.9)
    return {"adjacency": adjacency, "x_init": x_init, "teleport": teleport, "dangling": dangling, "damping": damping}


def reference(adjacency, x_init, teleport, dangling, damping):
    n_vert = adjacency.shape[0]
    dang_mask = dangling[:, None] > 0

    def sweep(x_cur, d_step):
        dang_mass = jnp.sum(jnp.where(dang_mask, x_cur, 0.0), axis=0)
        product = jnp.dot(adjacency, x_cur.astype(jnp.bfloat16), preferred_element_type=jnp.float32)
        x_next = d_step * product + (d_step * dang_mass / n_vert + (1.0 - d_step)) * teleport
        resid_row = jnp.sum(jnp.abs(x_next - x_cur), axis=0) / n_vert
        return x_next, resid_row

    x_final, residual = lax.scan(sweep, x_init, damping)
    return x_final, residual
```

```python
import functools

import jax
import jax.numpy as jnp
from jax import lax
from jax.experimental import pallas as pl
from jax.experimental.pallas import tpu as pltpu
from jax.sharding import PartitionSpec as P

F32, BF16, F8 = jnp.float32, jnp.bfloat16, jnp.float8_e4m3fn
NT = (((1,), (1,)), ((), ()))
N_CHUNK = 8
N_SUB = N_CHUNK // 2
LANES = 128


def kernel(
    n_vert, n_step,
    b_hbm, x_hbm, v_ref, w_ref, dang_ref, damp_ref,
    xo_ref, res_ref,
    b_ref, far_out, near_out, rx, ry, fwd, y_ref, xb_out, xb_in, mass_out, mass_in, coef, racc, macc,
    load_sem, far_sem, near_sem, rx_sem, ry_sem, fwd_sem, xbs_sem, xbr_sem, ms_sem, mr_sem,
):
    c = lax.axis_index("col")
    i = lax.axis_index("row")
    half_m, chunk = far_out.shape[2], far_out.shape[3]
    half_rows = N_CHUNK * chunk
    c_x = c + 1 - 2 * (c % 2)
    c_y = (c + 2) % 4
    c_d = 3 - c
    x_nbr = {"col": c_x, "row": i}
    y_nbr = {"col": c_y, "row": i}
    mate = {"col": c, "row": 1 - i}
    peers = [x_nbr, {"col": c_y, "row": 1 - i}, {"col": c_d, "row": 1 - i}]
    role = (c // 2 + i) % 2
    keeps = role == 0
    far_row = (1 - c % 2) * half_rows
    near_row = (c % 2) * half_rows

    def remote(src, dst, send, recv, dev):
        return pltpu.make_async_remote_copy(
            src_ref=src, dst_ref=dst, send_sem=send, recv_sem=recv, device_id=dev, device_id_type=pl.DeviceIdType.MESH
        )

    def product(h, row):
        rows = pl.ds(pl.multiple_of(row, chunk), chunk)
        both = lax.dot_general(y_ref[h], b_ref[rows, :], NT, preferred_element_type=F32)
        return both[:half_m] + both[half_m:]

    def set_y(h, j, xb):
        prod = xb.astype(F32) * w_ref[j]
        high = prod.astype(BF16)
        low = (prod - high.astype(F32)).astype(BF16)
        cols = pl.ds(pl.multiple_of(j * chunk, chunk), chunk)
        y_ref[h, :half_m, cols] = high
        y_ref[h, half_m:, cols] = low

    def far_copy(par, h, n, dev):
        return remote(far_out.at[h, n], rx.at[par, h, n], far_sem.at[h, n], rx_sem.at[par, h, n], dev)

    def hop_copy(par, h, n, k, dev):
        return remote(far_out.at[h, n], fwd.at[par, h, k], far_sem.at[h, n], fwd_sem.at[par, h, k], dev)

    def near_copy(par, h, n):
        return remote(near_out.at[h, n], ry.at[par, h, n], near_sem.at[h, n], ry_sem.at[par, h, n], y_nbr)

    def xb_copy(par, h, j):
        return remote(xb_out.at[h, j], xb_in.at[par, h, j], xbs_sem.at[h, j], xbr_sem.at[par, h, j], mate)

    def mass_copy(par, h, k):
        return remote(mass_out.at[h], mass_in.at[par, h, k], ms_sem.at[h, k], mr_sem.at[par, h, k], peers[k])

    def far(t, par, h, lo, hi):
        def step(it, carry):
            sub = (1 - role) * (it // N_SUB) + role * (1 - it % 2)
            k = (1 - role) * (it % N_SUB) + role * (it // 2)
            n = sub * N_SUB + k
            got = product(h, far_row + n * chunk)

            @pl.when(t > 0)
            def _():
                far_copy(par, h, n, x_nbr).wait_send()

            @pl.when(jnp.logical_and(keeps, sub == 1))
            def _():
                hop_copy(par, h, n, k, y_nbr).wait_recv()
                far_out[h, n] = got + fwd[par, h, k]

            @pl.when(jnp.logical_not(jnp.logical_and(keeps, sub == 1)))
            def _():
                far_out[h, n] = got

            @pl.when(keeps)
            def _():
                far_copy(par, h, n, x_nbr).start()

            @pl.when(jnp.logical_not(keeps))
            def _():
                dev = {"col": (1 - sub) * c_x + sub * c_y, "row": i}
                hop_copy(par, h, n, k, dev).start()

            return carry

        lax.fori_loop(lo, hi, step, 0)

    def near(t, par, h):
        def step(it, carry):
            sub = 1 - it // N_SUB
            k = it % N_SUB
            n = sub * N_SUB + k
            got = product(h, near_row + n * chunk)

            @pl.when(keeps)
            def _():
                near_out[h, n] = got

            @pl.when(jnp.logical_not(keeps))
            def _():
                @pl.when(t > 0)
                def _():
                    near_copy(par, h, n).wait_send()

                @pl.when(sub == 0)
                def _():
                    hop_copy(par, h, n, k, x_nbr).wait_recv()
                    near_out[h, n] = got + fwd[par, h, k]

                @pl.when(sub == 1)
                def _():
                    near_out[h, n] = got

                near_copy(par, h, n).start()

            return carry

        lax.fori_loop(0, N_CHUNK, step, 0)

    def lane_sums(acc):
        return jnp.sum(acc[...].T, axis=0, keepdims=True)

    def send_mass(par, h):
        mass_out[h] = jnp.broadcast_to(lane_sums(macc), mass_out.shape[1:])
        for k in range(3):
            mass_copy(par, h, k).start()

    def finalise(t, h):
        par = t % 2
        d = damp_ref[t]
        mass = mass_out[h]
        for k in range(3):
            mass_copy(par, h, k).wait()
            mass = mass + mass_in[par, h, k]
        spread = jnp.broadcast_to(mass[0:1], (LANES, LANES)).T
        coef[...] = d * spread[:half_m] / n_vert + (1.0 - d)
        racc[...] = jnp.zeros_like(racc)
        macc[...] = jnp.zeros_like(macc)

        def step(j, carry):
            far_copy(par, h, j, x_nbr).wait_recv()
            near_copy(par, h, j).wait_recv()

            @pl.when(t > 0)
            def _():
                xb_copy(par, h, j).wait_send()

            r_sum = racc[:half_m, :]
            m_sum = macc[:half_m, :]
            for g in range(chunk // LANES):
                at = pl.ds(g * LANES, LANES)
                total = near_out[h, j, :, at] + rx[par, h, j, :, at] + ry[par, h, j, :, at]
                new = d * total + coef[...] * v_ref[h, j, :, at]
                r_sum = r_sum + jnp.abs(new - xo_ref[h, j, :, at])
                m_sum = m_sum + jnp.where(dang_ref[j, :, at] > 0, new, 0.0)
                xo_ref[h, j, :, at] = new
                xb_out[h, j, :, at] = new.astype(BF16)
            racc[:half_m, :] = r_sum
            macc[:half_m, :] = m_sum

            @pl.when(t < n_step - 1)
            def _():
                xb_copy(1 - par, h, j).start()
                set_y(h, j, xb_out[h, j])

            return carry

        lax.fori_loop(0, N_CHUNK, step, 0)
        res_ref[h, pl.ds(t, 1), :] = lane_sums(racc) / n_vert

        @pl.when(t < n_step - 1)
        def _():
            send_mass(1 - par, h)

    b_load = pltpu.make_async_copy(b_hbm, b_ref, load_sem.at[0])
    x_load = pltpu.make_async_copy(x_hbm, xo_ref, load_sem.at[1])
    b_load.start()
    x_load.start()
    res_ref[...] = jnp.zeros_like(res_ref)
    x_load.wait()
    for h in range(2):
        def first(j, carry, h=h):
            set_y(h, j, xo_ref[h, j].astype(BF16))
            return carry

        lax.fori_loop(0, N_CHUNK, first, 0)

        @pl.when(keeps)
        def _(h=h):
            macc[...] = jnp.zeros_like(macc)

            def add(j, carry):
                m_sum = macc[:half_m, :]
                for g in range(chunk // LANES):
                    at = pl.ds(g * LANES, LANES)
                    m_sum = m_sum + jnp.where(dang_ref[j, :, at] > 0, xo_ref[h, j, :, at], 0.0)
                macc[:half_m, :] = m_sum
                return carry

            lax.fori_loop(0, N_CHUNK, add, 0)
            send_mass(0, h)

    b_load.wait()

    def sweep(t, carry):
        par = t % 2
        for h in range(2):
            @pl.when(jnp.logical_and(jnp.logical_not(keeps), t > 0))
            def _(h=h):
                def take(j, carry):
                    xb_copy(par, h, j).wait_recv()
                    set_y(h, j, xb_in[par, h, j])
                    return carry

                lax.fori_loop(0, N_CHUNK, take, 0)

            far(t, par, h, 0, N_SUB)
            if h == 0:
                @pl.when(jnp.logical_and(keeps, t > 0))
                def _():
                    finalise(t - 1, 1)
            else:
                @pl.when(keeps)
                def _():
                    finalise(t, 0)
            far(t, par, h, N_SUB, N_CHUNK)
            near(t, par, h)
        return carry

    lax.fori_loop(0, n_step, sweep, 0)

    @pl.when(keeps)
    def _():
        finalise(n_step - 1, 1)

    last = (n_step - 1) % 2
    for h in range(2):
        def drain(n, carry, h=h):
            far_copy(last, h, n, x_nbr).wait_send()

            @pl.when(jnp.logical_not(keeps))
            def _():
                near_copy(last, h, n).wait_send()

            return carry

        lax.fori_loop(0, N_CHUNK, drain, 0)


def solution(mesh):
    swap = [(0, 1), (1, 0)]

    def sweeps(adj_tile, x_piece, tele_piece, dang_piece, damping):
        tile_rows, tile_cols = adj_tile.shape
        piece, m = x_piece.shape
        n_vert = tile_rows * mesh.shape["row"]
        n_step = damping.shape[0]
        chunk, half_m = tile_cols // N_CHUNK, m // 2
        i = lax.axis_index("row")

        def both(own):
            other = lax.ppermute(own, "row", swap)
            return jnp.where(i == 0, jnp.concatenate([own, other]), jnp.concatenate([other, own]))

        def chunks(a):
            return a.reshape(N_CHUNK, chunk, 2, half_m).transpose(2, 0, 3, 1)

        top = jnp.max(adj_tile, axis=0).astype(F32)
        weight = jnp.maximum(top, lax.ppermute(top, "row", swap)).reshape(N_CHUNK, 1, chunk)
        edges = jnp.where(adj_tile > 0, 1.0, 0.0).astype(F8)
        x_in = chunks(both(x_piece))
        tele = chunks(both(tele_piece))
        dang = both(dang_piece).astype(F32).reshape(N_CHUNK, 1, chunk)

        part = (2, N_CHUNK, half_m, chunk)
        dma = pltpu.SemaphoreType.DMA
        vmem = pl.BlockSpec(memory_space=pltpu.VMEM)
        hbm = pl.BlockSpec(memory_space=pl.ANY)
        x_out, resid = pl.pallas_call(
            functools.partial(kernel, n_vert, n_step),
            out_shape=(jax.ShapeDtypeStruct(part, F32), jax.ShapeDtypeStruct((2, n_step, LANES), F32)),
            in_specs=[hbm, hbm, vmem, vmem, vmem, pl.BlockSpec(memory_space=pltpu.SMEM)],
            out_specs=(vmem, vmem),
            scratch_shapes=[
                pltpu.VMEM((tile_rows, tile_cols), F8),
                pltpu.VMEM(part, F32),
                pltpu.VMEM(part, F32),
                pltpu.VMEM((2, *part), F32),
                pltpu.VMEM((2, *part), F32),
                pltpu.VMEM((2, 2, N_SUB, half_m, chunk), F32),
                pltpu.VMEM((2, m, tile_cols), BF16),
                pltpu.VMEM(part, BF16),
                pltpu.VMEM((2, *part), BF16),
                pltpu.VMEM((2, 8, LANES), F32),
                pltpu.VMEM((2, 2, 3, 8, LANES), F32),
                pltpu.VMEM((half_m, LANES), F32),
                pltpu.VMEM((LANES, LANES), F32),
                pltpu.VMEM((LANES, LANES), F32),
                dma((2,)),
                dma((2, N_CHUNK)),
                dma((2, N_CHUNK)),
                dma((2, 2, N_CHUNK)),
                dma((2, 2, N_CHUNK)),
                dma((2, 2, N_SUB)),
                dma((2, N_CHUNK)),
                dma((2, 2, N_CHUNK)),
                dma((2, 3)),
                dma((2, 2, 3)),
            ],
            compiler_params=pltpu.CompilerParams(vmem_limit_bytes=67043328, has_side_effects=True),
            name="sweeps",
        )(edges, x_in, tele, weight, dang, damping)

        pieces = x_out.transpose(1, 3, 0, 2).reshape(2, piece, m)
        other = lax.ppermute(lax.dynamic_index_in_dim(pieces, 1 - i, 0, False), "row", swap)
        keeps = lax.axis_index("col") // 2 == i
        x_final = jnp.where(keeps, lax.dynamic_index_in_dim(pieces, i, 0, False), other)
        resid = lax.psum(resid[:, :, :half_m].transpose(1, 0, 2).reshape(n_step, m), ("col", "row"))
        return x_final, resid

    vec_spec = P(("col", "row"), None)
    return jax.shard_map(
        sweeps, mesh=mesh, in_specs=(P("row", "col"), vec_spec, vec_spec, P(("col", "row")), P()), out_specs=(vec_spec, P()), check_vma=False
    )
```

```python
import functools

import jax
import jax.numpy as jnp
from jax import lax
from jax.experimental import pallas as pl
from jax.experimental.pallas import tpu as pltpu
from jax.sharding import PartitionSpec as P

F32, BF16, F8 = jnp.float32, jnp.bfloat16, jnp.float8_e4m3fn
NT = (((1,), (1,)), ((), ()))
N_CHUNK = 8
N_SUB = N_CHUNK // 2
LANES = 128


def kernel(
    n_vert, n_step,
    a_hbm, x_hbm, v_hbm, dang_in, damp_ref,
    out_ref, res_ref,
    xo_ref, v_ref, dang_ref,
    b_ref, far_out, near_out, rx, ry, fwd, y_ref, xb_out, xb_in, mass_out, mass_in, coef, racc, macc,
    stage, w_own, w_in, w_ref, res_all, first_out,
    load_sem, w_sem, res_sem, ex_sem, end_sem, far_sem, near_sem, rx_sem, ry_sem, fwd_sem, xbs_sem, xbr_sem, ms_sem, mr_sem,
):
    c = lax.axis_index("col")
    i = lax.axis_index("row")
    half_m, chunk = far_out.shape[2], far_out.shape[3]
    half_rows = N_CHUNK * chunk
    c_x = c + 1 - 2 * (c % 2)
    c_y = (c + 2) % 4
    c_d = 3 - c
    x_nbr = {"col": c_x, "row": i}
    y_nbr = {"col": c_y, "row": i}
    mate = {"col": c, "row": 1 - i}
    peers = [x_nbr, {"col": c_y, "row": 1 - i}, {"col": c_d, "row": 1 - i}]
    role = (c // 2 + i) % 2
    keeps = role == 0
    far_row = (1 - c % 2) * half_rows
    near_row = (c % 2) * half_rows

    def remote(src, dst, send, recv, dev):
        return pltpu.make_async_remote_copy(
            src_ref=src, dst_ref=dst, send_sem=send, recv_sem=recv, device_id=dev, device_id_type=pl.DeviceIdType.MESH
        )

    def product(h, row):
        rows = pl.ds(pl.multiple_of(row, chunk), chunk)
        both = lax.dot_general(y_ref[h], b_ref[rows, :], NT, preferred_element_type=F32)
        return both[:half_m] + both[half_m:]

    def set_y(h, j, xb):
        prod = xb.astype(F32) * w_ref[j]
        high = prod.astype(BF16)
        low = (prod - high.astype(F32)).astype(BF16)
        cols = pl.ds(pl.multiple_of(j * chunk, chunk), chunk)
        y_ref[h, :half_m, cols] = high
        y_ref[h, half_m:, cols] = low

    def far_copy(par, h, n, dev):
        return remote(far_out.at[h, n], rx.at[par, h, n], far_sem.at[h, n], rx_sem.at[par, h, n], dev)

    def hop_copy(par, h, n, k, dev):
        return remote(far_out.at[h, n], fwd.at[par, h, k], far_sem.at[h, n], fwd_sem.at[par, h, k], dev)

    def near_copy(par, h, n):
        return remote(near_out.at[h, n], ry.at[par, h, n], near_sem.at[h, n], ry_sem.at[par, h, n], y_nbr)

    def xb_copy(par, h, j):
        return remote(xb_out.at[h, j], xb_in.at[par, h, j], xbs_sem.at[h, j], xbr_sem.at[par, h, j], mate)

    def mass_copy(par, h, k):
        return remote(mass_out.at[h], mass_in.at[par, h, k], ms_sem.at[h, k], mr_sem.at[par, h, k], peers[k])

    def far_place(it):
        sub = (1 - role) * (it // N_SUB) + role * (1 - it % 2)
        k = (1 - role) * (it % N_SUB) + role * (it // 2)
        return sub, k, sub * N_SUB + k

    def near_place(it):
        sub = 1 - it // N_SUB
        k = it % N_SUB
        return sub, k, sub * N_SUB + k

    def far(par, h, lo, hi):
        def step(it, carry):
            sub, k, n = far_place(it)
            got = product(h, far_row + n * chunk)
            far_copy(par, h, n, x_nbr).wait_send()
            emit_far(par, h, sub, k, n, got)
            return carry

        lax.fori_loop(lo, hi, step, 0)

    def emit_far(par, h, sub, k, n, got):
            @pl.when(jnp.logical_and(keeps, sub == 1))
            def _():
                hop_copy(par, h, n, k, y_nbr).wait_recv()
                far_out[h, n] = got + fwd[par, h, k]

            @pl.when(jnp.logical_not(jnp.logical_and(keeps, sub == 1)))
            def _():
                far_out[h, n] = got

            @pl.when(keeps)
            def _():
                far_copy(par, h, n, x_nbr).start()

            @pl.when(jnp.logical_not(keeps))
            def _():
                dev = {"col": (1 - sub) * c_x + sub * c_y, "row": i}
                hop_copy(par, h, n, k, dev).start()

    def near(par, h):
        def step(it, carry):
            sub, k, n = near_place(it)
            got = product(h, near_row + n * chunk)

            @pl.when(jnp.logical_not(keeps))
            def _():
                near_copy(par, h, n).wait_send()

            emit_near(par, h, sub, k, n, got)
            return carry

        lax.fori_loop(0, N_CHUNK, step, 0)

    def emit_near(par, h, sub, k, n, got):

            @pl.when(keeps)
            def _():
                near_out[h, n] = got

            @pl.when(jnp.logical_not(keeps))
            def _():
                @pl.when(sub == 0)
                def _():
                    hop_copy(par, h, n, k, x_nbr).wait_recv()
                    near_out[h, n] = got + fwd[par, h, k]

                @pl.when(sub == 1)
                def _():
                    near_out[h, n] = got

                near_copy(par, h, n).start()

    def lane_sums(acc):
        return jnp.sum(acc[...].T, axis=0, keepdims=True)

    def send_mass(par, h):
        mass_out[h] = jnp.broadcast_to(lane_sums(macc), mass_out.shape[1:])
        for k in range(3):
            mass_copy(par, h, k).start()

    def finalise(t, h):
        par = t % 2
        d = damp_ref[t]
        mass = mass_out[h]
        for k in range(3):
            mass_copy(par, h, k).wait()
            mass = mass + mass_in[par, h, k]
        spread = jnp.broadcast_to(mass[0:1], (LANES, LANES)).T
        coef[...] = d * spread[:half_m] / n_vert + (1.0 - d)
        racc[...] = jnp.zeros_like(racc)
        macc[...] = jnp.zeros_like(macc)

        def step(j, carry):
            far_copy(par, h, j, x_nbr).wait_recv()
            near_copy(par, h, j).wait_recv()

            @pl.when(t > 0)
            def _():
                xb_copy(par, h, j).wait_send()

            r_sum = racc[:half_m, :]
            m_sum = macc[:half_m, :]
            for g in range(chunk // LANES):
                at = pl.ds(g * LANES, LANES)
                total = near_out[h, j, :, at] + rx[par, h, j, :, at] + ry[par, h, j, :, at]
                new = d * total + coef[...] * v_ref[h, j, :, at]
                r_sum = r_sum + jnp.abs(new - xo_ref[h, j, :, at])
                m_sum = m_sum + jnp.where(dang_ref[j, :, at] > 0, new, 0.0)
                xo_ref[h, j, :, at] = new
                xb_out[h, j, :, at] = new.astype(BF16)
            racc[:half_m, :] = r_sum
            macc[:half_m, :] = m_sum

            @pl.when(t < n_step - 1)
            def _():
                xb_copy(1 - par, h, j).start()
                set_y(h, j, xb_out[h, j])

            return carry

        lax.fori_loop(0, N_CHUNK, step, 0)
        res_all[c, h, pl.ds(t, 1), :] = lane_sums(racc) / n_vert

        @pl.when(t < n_step - 1)
        def _():
            send_mass(1 - par, h)

    half = stage.shape[1]
    per = chunk // half

    def a_load(it):
        slab = it // per
        late = slab // N_CHUNK
        n_far, n_near = far_place(slab % N_CHUNK)[2], near_place(slab % N_CHUNK)[2]
        row = (1 - late) * (far_row + n_far * chunk) + late * (near_row + n_near * chunk)
        row = pl.multiple_of(row + (it % per) * half, half)
        return row, pltpu.make_async_copy(a_hbm.at[pl.ds(row, half), :], stage.at[it % 2], load_sem.at[it % 2])

    a_load(0)[1].start()
    w_own[...] = jnp.zeros_like(w_own)
    own = pl.ds(i * N_SUB, N_SUB)
    other = pl.ds((1 - i) * N_SUB, N_SUB)

    def swap(ref, k):
        return remote(ref, ref, ex_sem.at[0, k], ex_sem.at[1, k], mate)

    swaps = []
    for src, dst in ((x_hbm, xo_ref), (v_hbm, v_ref)):
        load = pltpu.make_async_copy(src, out_ref, load_sem.at[2])
        load.start()
        load.wait()

        def turn(n, carry, dst=dst):
            block = out_ref[pl.ds(pl.multiple_of(n * chunk, chunk), chunk), :].T
            dst[0, i * N_SUB + n] = block[:half_m]
            dst[1, i * N_SUB + n] = block[half_m:]
            return carry

        lax.fori_loop(0, N_SUB, turn, 0)
        for h in range(2):
            swaps.append(swap(dst.at[h, own], len(swaps)))
            swaps[-1].start()
    dang_ref[own] = dang_in[...]
    swaps.append(swap(dang_ref.at[own], len(swaps)))
    swaps[-1].start()
    for copy in swaps:
        copy.wait()
    for h in range(2):
        def first(j, carry, h=h):
            cols = pl.ds(pl.multiple_of(j * chunk, chunk), chunk)
            y_ref[0, h * half_m : (h + 1) * half_m, cols] = xo_ref[h, j].astype(BF16)
            return carry

        lax.fori_loop(0, N_CHUNK, first, 0)

        @pl.when(keeps)
        def _(h=h):
            macc[...] = jnp.zeros_like(macc)

            def add(j, carry):
                m_sum = macc[:half_m, :]
                for g in range(chunk // LANES):
                    at = pl.ds(g * LANES, LANES)
                    m_sum = m_sum + jnp.where(dang_ref[j, :, at] > 0, xo_ref[h, j, :, at], 0.0)
                macc[:half_m, :] = m_sum
                return carry

            lax.fori_loop(0, N_CHUNK, add, 0)
            send_mass(0, h)

    def slab(n_slab, emit, place):
        def step(it, carry):
            for e in range(per):
                at = (n_slab + it) * per + e
                row, load = a_load(at)
                load.wait()

                @pl.when(at + 1 < 2 * N_CHUNK * per)
                def _():
                    a_load(at + 1)[1].start()

                got = lax.dot_general(y_ref[0], stage[at % 2], NT, preferred_element_type=F32)
                first_out[:, e * half : (e + 1) * half] = got
                for j in range(N_CHUNK):
                    cols = slice(j * chunk, (j + 1) * chunk)
                    block = stage[at % 2, :, cols].astype(F32)
                    w_own[j] = jnp.maximum(w_own[j], jnp.max(block, axis=0, keepdims=True))
                    b_ref[pl.ds(row, half), cols] = jnp.where(block > 0, 1.0, 0.0).astype(F8)
            sub, k, n = place(it)
            for h in range(2):
                emit(0, h, sub, k, n, first_out[h * half_m : (h + 1) * half_m, :])
            return carry

        lax.fori_loop(0, N_CHUNK, step, 0)

    slab(0, emit_far, far_place)
    slab(N_CHUNK, emit_near, near_place)
    w_copy = remote(w_own, w_in, w_sem.at[0], w_sem.at[1], mate)
    w_copy.start()
    w_copy.wait()
    w_ref[...] = jnp.maximum(w_own[...], w_in[...])

    @pl.when(keeps)
    def _():
        finalise(0, 0)

    def sweep(t, carry):
        par = t % 2
        for h in range(2):
            @pl.when(jnp.logical_not(keeps))
            def _(h=h):
                def take(j, carry):
                    xb_copy(par, h, j).wait_recv()
                    set_y(h, j, xb_in[par, h, j])
                    return carry

                lax.fori_loop(0, N_CHUNK, take, 0)

            far(par, h, 0, N_SUB)

            @pl.when(keeps)
            def _(h=h):
                finalise(t - 1 + h, 1 - h)

            far(par, h, N_SUB, N_CHUNK)
            near(par, h)
        return carry

    lax.fori_loop(1, n_step, sweep, 0)

    @pl.when(keeps)
    def _():
        finalise(n_step - 1, 1)

    last = (n_step - 1) % 2
    for h in range(2):
        def drain(n, carry, h=h):
            far_copy(last, h, n, x_nbr).wait_send()

            @pl.when(jnp.logical_not(keeps))
            def _():
                near_copy(last, h, n).wait_send()

            return carry

        lax.fori_loop(0, N_CHUNK, drain, 0)

    def end_copy(h, piece):
        return remote(xo_ref.at[h, piece], xo_ref.at[h, piece], end_sem.at[0, h], end_sem.at[1, h], mate)

    @pl.when(keeps)
    def _():
        for h in range(2):
            end_copy(h, other).start()
        for h in range(2):
            end_copy(h, other).wait_send()

    @pl.when(jnp.logical_not(keeps))
    def _():
        for h in range(2):
            end_copy(h, own).wait_recv()

    def turn_back(n, carry):
        block = jnp.concatenate([xo_ref[0, i * N_SUB + n], xo_ref[1, i * N_SUB + n]], axis=0)
        out_ref[pl.ds(pl.multiple_of(n * chunk, chunk), chunk), :] = block.T
        return carry

    lax.fori_loop(0, N_SUB, turn_back, 0)

    def res_copy(k):
        return remote(res_all.at[c], res_all.at[c], res_sem.at[k], res_sem.at[3 + k], peers[k])

    total_copy = remote(res_ref, res_ref, res_sem.at[6], res_sem.at[7], mate)

    @pl.when(keeps)
    def _():
        for k in range(3):
            res_copy(k).start()
        for k in range(3):
            res_copy(k).wait()
        res_ref[...] = res_all[0] + res_all[1] + res_all[2] + res_all[3]
        total_copy.start()
        total_copy.wait_send()

    @pl.when(jnp.logical_not(keeps))
    def _():
        total_copy.wait_recv()


def solution(mesh):
    def sweeps(adj_tile, x_piece, tele_piece, dang_piece, damping):
        tile_rows, tile_cols = adj_tile.shape
        piece, m = x_piece.shape
        n_vert = tile_rows * mesh.shape["row"]
        n_step = damping.shape[0]
        chunk, half_m = tile_cols // N_CHUNK, m // 2
        dang = dang_piece.astype(F32).reshape(N_SUB, 1, chunk)

        part = (2, N_CHUNK, half_m, chunk)
        dma = pltpu.SemaphoreType.DMA
        vmem = pl.BlockSpec(memory_space=pltpu.VMEM)
        hbm = pl.BlockSpec(memory_space=pl.ANY)
        x_final, resid = pl.pallas_call(
            functools.partial(kernel, n_vert, n_step),
            out_shape=(jax.ShapeDtypeStruct((piece, m), F32), jax.ShapeDtypeStruct((2, n_step, LANES), F32)),
            in_specs=[hbm, hbm, hbm, vmem, pl.BlockSpec(memory_space=pltpu.SMEM)],
            out_specs=(vmem, vmem),
            scratch_shapes=[
                pltpu.VMEM(part, F32),
                pltpu.VMEM(part, F32),
                pltpu.VMEM((N_CHUNK, 1, chunk), F32),
                pltpu.VMEM((tile_rows, tile_cols), F8),
                pltpu.VMEM(part, F32),
                pltpu.VMEM(part, F32),
                pltpu.VMEM((2, *part), F32),
                pltpu.VMEM((2, *part), F32),
                pltpu.VMEM((2, 2, N_SUB, half_m, chunk), F32),
                pltpu.VMEM((2, m, tile_cols), BF16),
                pltpu.VMEM(part, BF16),
                pltpu.VMEM((2, *part), BF16),
                pltpu.VMEM((2, 8, LANES), F32),
                pltpu.VMEM((2, 2, 3, 8, LANES), F32),
                pltpu.VMEM((half_m, LANES), F32),
                pltpu.VMEM((LANES, LANES), F32),
                pltpu.VMEM((LANES, LANES), F32),
                pltpu.VMEM((2, chunk // 2, tile_cols), BF16),
                pltpu.VMEM((N_CHUNK, 1, chunk), F32),
                pltpu.VMEM((N_CHUNK, 1, chunk), F32),
                pltpu.VMEM((N_CHUNK, 1, chunk), F32),
                pltpu.VMEM((4, 2, n_step, LANES), F32),
                pltpu.VMEM((m, chunk), F32),
                dma((3,)),
                dma((2,)),
                dma((8,)),
                dma((2, 5)),
                dma((2, 2)),
                dma((2, N_CHUNK)),
                dma((2, N_CHUNK)),
                dma((2, 2, N_CHUNK)),
                dma((2, 2, N_CHUNK)),
                dma((2, 2, N_SUB)),
                dma((2, N_CHUNK)),
                dma((2, 2, N_CHUNK)),
                dma((2, 3)),
                dma((2, 2, 3)),
            ],
            compiler_params=pltpu.CompilerParams(vmem_limit_bytes=67043328, has_side_effects=True),
            name="sweeps",
        )(adj_tile, x_piece, tele_piece, dang, damping)

        resid = resid[:, :, :half_m].transpose(1, 0, 2).reshape(n_step, m)
        return x_final, resid

    vec_spec = P(("col", "row"), None)
    return jax.shard_map(
        sweeps, mesh=mesh, in_specs=(P("row", "col"), vec_spec, vec_spec, P(("col", "row")), P()), out_specs=(vec_spec, P()), check_vma=False
    )
```
